32 devices in a mesh: intra: 4 (over y, x), inter: 8 (over z, core).
Axes of the slice: x: 2, y: 2, z: 4, core: 2. Of those that a mesh axis runs over, the one named last changes fastest.
Arguments:
- gate_pre: bfloat16 [1536, 14336], P('intra', 'inter'), may hold values from -6 to 6
- up_pre: bfloat16 [1536, 14336], P('intra', 'inter'), may hold values from -6 to 6
- cotangent: bfloat16 [1536, 8192], P('intra'), may hold values from -6 to 6
- weight_codes: bfloat16 [8192, 14336], P('intra', 'inter'), may hold values from -0.0625 to 0.0625
- weight_scale: bfloat16 [128, 14336], P('intra', 'inter'), may hold values from 0.5 to 2
- section_one: float32 [128, 14336], P(None, 'inter'), may hold values from 1 to 20
- section_two: float32 [128, 14336], P('intra', 'inter'), may hold values from 4 to 60
Outputs:
- grad_gate: bfloat16 [1536, 14336], P('intra', 'inter')
- grad_up: bfloat16 [1536, 14336], P('intra', 'inter')
- grad_codes: float32 [8192, 14336], P(('intra', 'inter'))
The draws below stay inside these ranges and needn't reach their ends.
All inputs are finite; a program needn't handle non-finite values.
Results may differ from the reference program's by a relative error of at most 0.015.
Values may be sent and summed in bfloat16 or wider, within the bound.
A program may use at most 256 MiB of HBM per device.

```python
import math
import jax
import jax.numpy as jnp
from jax import lax

D = 8192
FW = 14336
BLK = 64
TOK_DEV = 384
TOKENS = 1536
NB = 128
N_INTRA = 4


def block_levels(stream_key, dims, shards, smallest, high):
    def one(dim, shards_of):
        steps = jax.random.uniform(jax.random.fold_in(jax.random.fold_in(stream_key, 6), dim), (shards_of,), jnp.float32, smallest / len(shards), high / len(shards))
        return jnp.repeat(jnp.exp(steps), dims[dim] // shards_of).reshape((-1,) + (1,) * (len(dims) - dim - 1))

    factor_of = one(*shards[0])
    for cut in shards[1:]:
        factor_of = factor_of * one(*cut)
    return factor_of


def bell_draw(stream_key, shape, width, bound, split=(), kind=jnp.bfloat16):
    entries = width * jax.random.normal(stream_key, shape, jnp.float32)
    if split:
        entries = entries * block_levels(stream_key, shape, split, -0.22, 0.18)
    return jnp.clip(entries, -bound, bound).astype(kind)


def setup_inputs(seed: int = 0) -> dict:
    streams_of = jax.random.split(jax.random.key(seed), 8)
    return {
        "gate_pre": bell_draw(streams_of[0], (TOKENS, FW), 1.0, 6.0, ((0, 4), (1, 8))),
        "up_pre": bell_draw(streams_of[1], (TOKENS, FW), 1.0, 6.0, ((0, 4), (1, 8))),
        "cotangent": bell_draw(streams_of[2], (TOKENS, D), 1.0, 6.0, ((0, 4),)),
        "weight_codes": bell_draw(streams_of[3], (D, FW), D ** -0.5, 0.0625, ((0, 4), (1, 8))),
        "weight_scale": jnp.clip(jnp.exp(math.log(2.0) - 1.3862944 * jax.random.uniform(streams_of[4], (NB, FW), jnp.float32) ** block_levels(streams_of[4], (NB, FW), ((0, 4), (1, 8)), -0.2, 0.2)), 0.5, 2.0).astype(jnp.bfloat16),
        "section_one": jnp.clip(jnp.exp(math.log(20.0) - 2.9957323 * jax.random.uniform(streams_of[5], (NB, FW), jnp.float32) ** block_levels(streams_of[5], (NB, FW), ((1, 8),), -0.2, 0.2)), 1.0, 20.0),
        "section_two": jnp.clip(jnp.exp(math.log(60.0) - 2.7080502 * jax.random.uniform(streams_of[6], (NB, FW), jnp.float32) ** block_levels(streams_of[6], (NB, FW), ((0, 4), (1, 8)), -0.2, 0.2)), 4.0, 60.0),
    }


def soft_code(values):
    return 7.0 * jnp.tanh(values / 7.0)


def expand(scales):
    return jnp.repeat(scales, BLK, axis=0)


def reference(gate_pre, up_pre, cotangent, weight_codes, weight_scale, section_one, section_two):
    layer = (weight_codes.astype(jnp.float32) * expand(weight_scale).astype(jnp.float32)).astype(jnp.bfloat16)
    one_full = expand(section_one)
    two_full = expand(section_two)

    def block_step(total, block_index):
        start = (block_index * TOK_DEV).astype(jnp.int32)
        rows_out = lax.dynamic_slice_in_dim(cotangent, start, TOK_DEV, 0)
        gate_rows = lax.dynamic_slice_in_dim(gate_pre, start, TOK_DEV, 0).astype(jnp.float32)
        up_rows = lax.dynamic_slice_in_dim(up_pre, start, TOK_DEV, 0).astype(jnp.float32)
        sigma = jax.nn.sigmoid(gate_rows)
        gated = gate_rows * sigma
        hidden = (gated * up_rows).astype(jnp.bfloat16)
        grad_hidden = jnp.dot(rows_out, layer, preferred_element_type=jnp.float32)
        grad_gate = (grad_hidden * up_rows * sigma * (1.0 + gate_rows * (1.0 - sigma))).astype(jnp.bfloat16)
        grad_up = (grad_hidden * gated).astype(jnp.bfloat16)
        term = jnp.dot(rows_out.T, hidden, preferred_element_type=jnp.float32)
        coded = lax.optimization_barrier(soft_code(term / one_full).astype(jnp.bfloat16))
        return total + coded.astype(jnp.float32), (grad_gate, grad_up)

    first, grads = lax.scan(block_step, jnp.zeros((D, FW), jnp.float32), jnp.arange(N_INTRA, dtype=jnp.int32))
    second = soft_code(first * one_full / two_full).astype(jnp.bfloat16).astype(jnp.float32)
    grad_gate = grads[0].reshape(TOK_DEV * N_INTRA, FW)
    grad_up = grads[1].reshape(TOK_DEV * N_INTRA, FW)
    return grad_gate, grad_up, second
```

```python
import functools

import jax
import jax.numpy as jnp
from jax import lax
from jax.experimental import pallas as pl
from jax.experimental.pallas import tpu as pltpu
from jax.sharding import PartitionSpec as P

MESH = pl.DeviceIdType.MESH
LANES = 128
PIECE = 512


def times(n, x):
    return pl.multiple_of(x, n)


def bits_below(n):
    return [1 << k for k in range(n.bit_length() - 1)]


def xor(x, y, n):
    out = 0
    for bit in bits_below(n):
        one = lax.rem(lax.div(x, jnp.int32(bit)) + lax.div(jnp.int32(y), jnp.int32(bit)), jnp.int32(2))
        out = out + bit * one
    return out


def combos(masks):
    out = [0]
    for mask in masks:
        out = out + [c ^ mask for c in out]
    return out


def pieces(lo, hi, most=PIECE):
    out = []
    while lo < hi:
        out.append((lo, min(most, hi - lo)))
        lo += most
    return out


class Plan:
    def __init__(self, tok, model, width, rows, n_blocks, n_intra, n_inter):
        self.tok, self.model, self.width, self.rows = tok, model, width, rows
        self.blocks, self.blk = n_blocks, rows // n_blocks
        self.n_intra, self.n_inter = n_intra, n_inter
        self.own = rows // n_inter
        lanes = width // LANES
        self.swap = (lanes + 1) // 2 * LANES
        self.keep = width - self.swap
        self.wide = width + self.swap
        self.half = n_inter // 2
        self.near_rows = rows // 2
        self.quarter = rows // 4
        self.tile = max(self.own, LANES)
        self.share = [2, 1]
        self.n_share = 4
        self.dims = bits_below(n_intra)
        self.far_cols = pieces(0, self.keep)
        self.home_cols = pieces(self.keep, width)
        self.swap_cols = pieces(width, self.wide)
        self.hidden_cols = self.far_cols + self.home_cols + self.swap_cols
        self.sum_cols = pieces(0, width)

    def order(self, color):
        return self.dims[color:] + self.dims[:color]


def remote(src, dst, send, recv, device):
    return pltpu.make_async_remote_copy(
        src_ref=src, dst_ref=dst, send_sem=send, recv_sem=recv, device_id=device, device_id_type=MESH
    )


def main_kernel(
    plan,
    gate_hbm, up_hbm, cot_hbm, codes_hbm, scale_hbm, one_hbm, two_hbm,
    got_hbm, dgate_hbm, dup_hbm,
    gate, up, hid, cols, codes, scale, lay, inv, ratio, coded, part, sums,
    load_sem, xy_sem, share_sem, swap_sem, gather_sem, sum_sem, out_sem, own_sem, store_sem,
):
    p = plan
    i = lax.axis_index("intra")
    b = lax.axis_index("inter")
    n_a, n_b, tok = p.n_intra, p.n_inter, p.tok
    side = lax.div(b, jnp.int32(p.half))
    share_at = lax.rem(b, jnp.int32(p.n_share))
    part_tok = tok // p.n_share
    colors = len(p.dims)
    color_tok = tok // colors
    ia = functools.partial(xor, i, n=n_a)
    ib = functools.partial(xor, b, n=n_b)

    loads = [
        pltpu.make_async_copy(gate_hbm, gate, load_sem.at[0]),
        pltpu.make_async_copy(up_hbm, up, load_sem.at[1]),
        pltpu.make_async_copy(
            one_hbm.at[pl.ds(times(8, i * p.blocks), p.blocks)], inv.at[:, :p.width], load_sem.at[2]
        ),
        pltpu.make_async_copy(two_hbm, ratio.at[:, :p.width], load_sem.at[3]),
        pltpu.make_async_copy(
            cot_hbm.at[:, pl.ds(times(LANES, i * p.rows), p.rows)],
            cols.at[pl.ds(times(tok, i * tok), tok)],
            load_sem.at[4],
        ),
        pltpu.make_async_copy(codes_hbm, codes, load_sem.at[5]),
        pltpu.make_async_copy(scale_hbm, scale, load_sem.at[6]),
    ]
    for load in loads:
        load.start()

    barrier = pltpu.get_barrier_semaphore()
    for a in range(1, n_a):
        pl.semaphore_signal(barrier, inc=1, device_id=(ia(a), b), device_id_type=MESH)
    for a in range(1, n_b):
        pl.semaphore_signal(barrier, inc=1, device_id=(i, ib(a)), device_id_type=MESH)
    pl.semaphore_wait(barrier, n_a - 1 + n_b - 1)

    def row_start(step):
        toward = (1 - side) if step < 2 else side
        return times(LANES, toward * p.near_rows + (step % 2) * p.quarter)

    def across(step, a, sending):
        peer = ia(a)
        r0 = row_start(step)
        block = i if sending else peer
        src = cot_hbm.at[
            pl.ds(times(16, share_at * part_tok), part_tok),
            pl.ds(times(LANES, peer * p.rows + r0), p.quarter),
        ]
        dst = cols.at[
            pl.ds(times(16, block * tok + share_at * part_tok), part_tok), pl.ds(r0, p.quarter)
        ]
        k = step * (n_a - 1) + a - 1
        return remote(src, dst, xy_sem.at[0, k], xy_sem.at[1, k], (peer, b))

    def start_across(step):
        for a in range(1, n_a):
            across(step, a, True).start()

    def wait_across(step):
        for a in range(1, n_a):
            across(step, a, False).wait_recv()

    def shares(step, phase, sending):
        mask = p.share[phase]
        peer = ib(mask)
        r0 = row_start(step)
        out = []
        for a in range(1, n_a):
            for n, c in enumerate(combos(p.share[:phase])):
                at = xor(share_at, c if sending else c ^ mask, p.n_share)
                ref = cols.at[
                    pl.ds(times(16, ia(a) * tok + at * part_tok), part_tok), pl.ds(r0, p.quarter)
                ]
                k = (step * (n_a - 1) + a - 1) * (p.n_share - 1) + (1 << phase) - 1 + n
                out.append(remote(ref, ref, share_sem.at[0, k], share_sem.at[1, k], (i, peer)))
        return out

    def start_shares(step, phase):
        for copy in shares(step, phase, True):
            copy.start()

    def wait_shares(step, phase):
        for copy in shares(step, phase, False):
            copy.wait_recv()

    def gathers(piece, phase, sending):
        c0, w = p.hidden_cols[piece]
        out = []
        for color in range(colors):
            order = p.order(color)
            mask = order[phase]
            for n, c in enumerate(combos(order[:phase])):
                block = ia(c if sending else c ^ mask)
                ref = hid.at[
                    pl.ds(times(16, block * tok + color * color_tok), color_tok), c0:c0 + w
                ]
                k = (piece * colors + color) * (n_a - 1) + (1 << phase) - 1 + n
                out.append(remote(ref, ref, gather_sem.at[0, k], gather_sem.at[1, k], (ia(mask), b)))
        return out

    def start_gather(piece, phase):
        for copy in gathers(piece, phase, True):
            copy.start()

    def wait_gather(piece, phase):
        for copy in gathers(piece, phase, False):
            copy.wait_recv()

    def rest_of_gather(piece, phase):
        for q in range(phase, len(p.dims)):
            wait_gather(piece, q)
            if q + 1 < len(p.dims):
                start_gather(piece, q + 1)

    def make_hidden(piece):
        c0, w = p.hidden_cols[piece]
        step_tok = 64

        def body(t, carry):
            rows = pl.ds(times(step_tok, t * step_tok), step_tok)
            g = gate[rows, c0:c0 + w].astype(jnp.float32)
            u = up[rows, c0:c0 + w].astype(jnp.float32)
            h = g * jax.nn.sigmoid(g) * u
            hid[pl.ds(times(step_tok, i * tok + t * step_tok), step_tok), c0:c0 + w] = h.astype(hid.dtype)
            return carry

        lax.fori_loop(0, tok // step_tok, body, 0)

    n_half = p.blocks // 2

    def swaps(sending):
        other = ib(p.half)
        at = (1 - side) if sending else side
        rows = pl.ds(times(8, at * n_half), n_half)
        block = pl.ds(times(tok, i * tok), tok)
        out = []
        k = 0
        for buf, sel in ((hid, block), (inv, rows), (ratio, rows)):
            out.append(
                remote(
                    buf.at[sel, p.keep:p.width], buf.at[sel, p.width:p.wide],
                    swap_sem.at[0, k], swap_sem.at[1, k], (i, other),
                )
            )
            k += 1
        return out

    def prepare_scales():
        one = inv[:, :p.width]
        ratio[:, :p.width] = one / ratio[:, :p.width]
        inv[:, :p.width] = 1.0 / (7.0 * one)

    n_pieces = len(p.hidden_cols)
    per = p.tile // p.own

    def out_copy(owner, piece):
        c0, w = p.hidden_cols[piece]
        if c0 < p.width:
            source, at = b, c0
        else:
            source, at = ib(p.half), c0 - p.swap
        rel = ib(owner)
        k = rel * n_pieces + piece
        return remote(
            coded.at[pl.ds(times(16, owner * p.own), p.own), c0:c0 + w],
            got_hbm.at[source, :, at:at + w],
            out_sem.at[0, k], out_sem.at[1, k], (i, owner),
        )

    def own_copy(piece):
        c0, w = p.hidden_cols[piece]
        if c0 < p.width:
            source, at = b, c0
        else:
            source, at = ib(p.half), c0 - p.swap
        return pltpu.make_async_copy(
            coded.at[pl.ds(times(16, b * p.own), p.own), c0:c0 + w],
            got_hbm.at[source, :, at:at + w],
            own_sem.at[piece],
        )

    def make_coded(step, piece):
        c0, w = p.hidden_cols[piece]
        r0 = row_start(step)

        def body(t, carry):
            start = times(p.tile, r0 + t * p.tile)
            total = [None] * (p.tile // p.blk)
            for a in range(n_a):
                term = lax.dot_general(
                    cols[a * tok:(a + 1) * tok, pl.ds(start, p.tile)],
                    hid[a * tok:(a + 1) * tok, c0:c0 + w],
                    (((0,), (0,)), ((), ())),
                    preferred_element_type=jnp.float32,
                )
                for q in range(p.tile // p.blk):
                    at = lax.div(start, jnp.int32(p.blk)) + q
                    v = jnp.tanh(term[q * p.blk:(q + 1) * p.blk] * inv[pl.ds(at, 1), c0:c0 + w])
                    total[q] = v if a == 0 else total[q] + v
            for q in range(p.tile // p.blk):
                at = lax.div(start, jnp.int32(p.blk)) + q
                second = 7.0 * jnp.tanh(total[q] * ratio[pl.ds(at, 1), c0:c0 + w])
                coded[pl.ds(times(p.blk, start + q * p.blk), p.blk), c0:c0 + w] = second.astype(coded.dtype)
            for o in range(per):
                owner = lax.div(start, jnp.int32(p.own)) + o

                @pl.when(owner == b)
                def _():
                    own_copy(piece).start()

                @pl.when(owner != b)
                def _():
                    out_copy(owner, piece).start()
            return carry

        lax.fori_loop(0, p.quarter // p.tile, body, 0)

    sub = 256 if all(w % 256 == 0 for _, w in p.sum_cols) else LANES

    def make_partial(piece):
        c0, w = p.sum_cols[piece]

        def body(t, carry):
            at = times(LANES, c0 + t * sub)

            def scaled(n, inner):
                rows = pl.ds(times(p.blk, n * p.blk), p.blk)
                lay[rows, :] = (
                    codes[rows, pl.ds(at, sub)].astype(jnp.float32)
                    * scale[pl.ds(n, 1), pl.ds(at, sub)].astype(jnp.float32)
                ).astype(lay.dtype)
                return inner

            for n in range(p.blocks):
                scaled(n, 0)

            def block(a, inner):
                rows = pl.ds(times(tok, a * tok), tok)
                part[rows, pl.ds(at, sub)] = jnp.dot(
                    cols[rows, :], lay[...], preferred_element_type=jnp.float32
                ).astype(part.dtype)
                return inner

            lax.fori_loop(0, n_a, block, 0)
            return carry

        lax.fori_loop(0, w // sub, body, 0)

    def sum_copies(piece, phase, sending):
        c0, w = p.sum_cols[piece]
        out = []
        for color in range(colors):
            order = p.order(color)
            mask = order[phase]
            base = n_a - (n_a >> phase)
            for n, c in enumerate(combos(order[phase + 1:])):
                src = part.at[
                    pl.ds(times(16, ia(c ^ mask) * tok + color * color_tok), color_tok), c0:c0 + w
                ]
                dst = sums.at[
                    (base + n) * tok + color * color_tok:(base + n) * tok + (color + 1) * color_tok,
                    c0:c0 + w,
                ]
                k = (piece * colors + color) * (n_a - 1) + base + n
                out.append(
                    (remote(src, dst, sum_sem.at[0, k], sum_sem.at[1, k], (ia(mask), b)), color, base + n, c)
                )
        return out

    def start_sum(piece, phase):
        for copy, *_ in sum_copies(piece, phase, True):
            copy.start()

    def finish_sum(piece, phase):
        c0, w = p.sum_cols[piece]
        last = phase + 1 == len(p.dims)
        step_tok = 32
        for copy, color, slot, c in sum_copies(piece, phase, False):
            copy.wait_recv()

            def body(t, carry):
                mine = pl.ds(times(16, ia(c) * tok + color * color_tok + t * step_tok), step_tok)
                theirs = pl.ds(times(16, slot * tok + color * color_tok + t * step_tok), step_tok)
                both = part[mine, c0:c0 + w].astype(jnp.float32) + sums[theirs, c0:c0 + w].astype(jnp.float32)
                if not last:
                    part[mine, c0:c0 + w] = both.astype(part.dtype)
                else:
                    here = pl.ds(times(16, color * color_tok + t * step_tok), step_tok)
                    g = gate[here, c0:c0 + w].astype(jnp.float32)
                    u = up[here, c0:c0 + w].astype(jnp.float32)
                    sigma = jax.nn.sigmoid(g)
                    gate[here, c0:c0 + w] = (both * u * sigma * (1.0 + g * (1.0 - sigma))).astype(gate.dtype)
                    up[here, c0:c0 + w] = (both * (g * sigma)).astype(up.dtype)
                return carry

            lax.fori_loop(0, color_tok // step_tok, body, 0)
        if not last:
            start_sum(piece, phase + 1)
        else:
            for copy in stores(piece):
                copy.start()

    def stores(piece):
        c0, w = p.sum_cols[piece]
        return [
            pltpu.make_async_copy(src.at[:, c0:c0 + w], dst.at[:, c0:c0 + w], store_sem.at[2 * piece + n])
            for n, (src, dst) in enumerate(((gate, dgate_hbm), (up, dup_hbm)))
        ]

    far = list(range(len(p.far_cols)))
    home = [len(far) + n for n in range(len(p.home_cols))]
    swapped = [len(far) + len(home) + n for n in range(len(p.swap_cols))]
    n_sum = len(p.sum_cols)
    first, later = (far + home)[0], (far + home)[1:]
    later_far = [x for x in far if x != first]

    loads[0].wait()
    loads[1].wait()
    start_across(0)
    make_hidden(first)
    start_gather(first, 0)
    start_across(1)
    for x in home:
        make_hidden(x)
    for x in later_far:
        make_hidden(x)
    loads[2].wait()
    loads[3].wait()
    prepare_scales()
    loads[4].wait()
    wait_across(0)
    start_shares(0, 0)
    rest_of_gather(first, 0) if len(p.dims) == 1 else wait_gather(first, 0)
    if len(p.dims) > 1:
        start_gather(first, 1)
    start_across(2)
    start_across(3)
    wait_across(1)
    start_shares(1, 0)
    wait_shares(0, 0)
    start_shares(0, 1)
    for copy in swaps(True):
        copy.start()
    wait_shares(1, 0)
    start_shares(1, 1)
    for x in later:
        start_gather(x, 0)
    wait_across(2)
    start_shares(2, 0)
    rest_of_gather(first, 1)
    wait_shares(0, 1)
    make_coded(0, first)
    wait_across(3)
    start_shares(3, 0)
    wait_shares(2, 0)
    start_shares(2, 1)
    wait_shares(1, 1)
    make_coded(1, first)
    for x in later_far:
        wait_gather(x, 0)
        if len(p.dims) > 1:
            start_gather(x, 1)
    wait_shares(3, 0)
    start_shares(3, 1)
    wait_shares(2, 1)
    make_coded(2, first)
    wait_shares(3, 1)
    make_coded(3, first)
    for x in home:
        wait_gather(x, 0)
        if len(p.dims) > 1:
            start_gather(x, 1)
    for copy in swaps(False):
        copy.wait_recv()
    for x in swapped:
        start_gather(x, 0)
    for x in later_far:
        rest_of_gather(x, 1)
        for step in range(4):
            make_coded(step, x)
    loads[5].wait()
    loads[6].wait()
    make_partial(0)
    for x in swapped:
        wait_gather(x, 0)
        if len(p.dims) > 1:
            start_gather(x, 1)
    start_sum(0, 0)
    for x in home:
        rest_of_gather(x, 1)
        for step in (2, 3):
            make_coded(step, x)
    for n in range(1, n_sum):
        make_partial(n)
        start_sum(n, 0)
    for x in swapped:
        rest_of_gather(x, 1)
        for step in (2, 3):
            make_coded(step, x)
    for phase in range(len(p.dims)):
        for n in range(n_sum):
            finish_sum(n, phase)

    for n in range(n_sum):
        for copy in stores(n):
            copy.wait()
    for x in range(n_pieces):
        own_copy(x).wait()
        for rel in range(1, n_b if x in far else p.half):
            owner = ib(rel)
            copy = out_copy(owner, x)
            copy.wait_recv()
            copy.wait_send()
    for step in range(4):
        for a in range(1, n_a):
            across(step, a, True).wait_send()
        for phase in range(len(p.share)):
            for copy in shares(step, phase, True):
                copy.wait_send()
    for copy in swaps(True):
        copy.wait_send()
    for phase in range(len(p.dims)):
        for x in range(n_pieces):
            for copy in gathers(x, phase, True):
                copy.wait_send()
        for n in range(n_sum):
            for copy, *_ in sum_copies(n, phase, True):
                copy.wait_send()


def main_call(plan, gate, up, cot, codes, scale, one, two):
    p = plan
    bf16, f32 = jnp.bfloat16, jnp.float32
    vmem, dma = pltpu.VMEM, pltpu.SemaphoreType.DMA
    everywhere = pl.BlockSpec(memory_space=pl.ANY)
    gather = len(p.dims) * (p.n_intra - 1)
    flops = 4 * p.rows * p.width * p.n_intra * p.tok
    return pl.pallas_call(
        functools.partial(main_kernel, p),
        in_specs=[everywhere] * 7,
        out_specs=[everywhere] * 3,
        out_shape=[
            jax.ShapeDtypeStruct((p.n_inter, p.own, p.width), bf16),
            jax.ShapeDtypeStruct((p.tok, p.width), bf16),
            jax.ShapeDtypeStruct((p.tok, p.width), bf16),
        ],
        scratch_shapes=[
            vmem((p.tok, p.width), bf16),
            vmem((p.tok, p.width), bf16),
            vmem((p.n_intra * p.tok, p.wide), bf16),
            vmem((p.n_intra * p.tok, p.rows), bf16),
            vmem((p.rows, p.width), bf16),
            vmem((p.blocks, p.width), bf16),
            vmem((p.rows, 256 if all(w % 256 == 0 for _, w in p.sum_cols) else LANES), bf16),
            vmem((p.blocks, p.wide), f32),
            vmem((p.blocks, p.wide), f32),
            vmem((p.rows, p.wide), bf16),
            vmem((p.n_intra * p.tok, p.width), bf16),
            vmem(((p.n_intra - 1) * p.tok, p.width), bf16),
            dma((7,)),
            dma((2, 4 * (p.n_intra - 1))),
            dma((2, 4 * (p.n_intra - 1) * (p.n_share - 1))),
            dma((2, 3)),
            dma((2, len(p.hidden_cols) * gather)),
            dma((2, len(p.sum_cols) * gather)),
            dma((2, p.n_inter * len(p.hidden_cols))),
            dma((len(p.hidden_cols),)),
            dma((2 * len(p.sum_cols),)),
        ],
        cost_estimate=pl.CostEstimate(
            flops=flops, bytes_accessed=2 * flops // p.tok, transcendentals=5 * p.rows * p.width
        ),
        compiler_params=pltpu.CompilerParams(
            collective_id=0, has_side_effects=True, vmem_limit_bytes=63 * 2**20
        ),
    )(gate, up, cot, codes, scale, one, two)


def join_kernel(got, dgate, dup, codes_out, dgate_out, dup_out):
    codes_out[...] = got[...].astype(jnp.float32)
    dgate_out[...] = dgate[...]
    dup_out[...] = dup[...]


def join_call(got, dgate, dup):
    sources, rows, width = got.shape
    tok = dgate.shape[0]
    grads = pl.BlockSpec((tok // sources, width), lambda j: (j, 0))
    return pl.pallas_call(
        join_kernel,
        grid=(sources,),
        in_specs=[pl.BlockSpec((None, rows, width), lambda j: (j, 0, 0)), grads, grads],
        out_specs=[pl.BlockSpec((rows, width), lambda j: (0, j)), grads, grads],
        out_shape=[
            jax.ShapeDtypeStruct((rows, sources * width), jnp.float32),
            jax.ShapeDtypeStruct(dgate.shape, dgate.dtype),
            jax.ShapeDtypeStruct(dup.shape, dup.dtype),
        ],
        cost_estimate=pl.CostEstimate(
            flops=0, bytes_accessed=6 * got.size + 8 * dgate.size, transcendentals=0
        ),
        compiler_params=pltpu.CompilerParams(vmem_limit_bytes=24 * 2**20),
    )(got, dgate, dup)


def on_device(gate_pre, up_pre, cotangent, weight_codes, weight_scale, section_one, section_two):
    plan = Plan(
        cotangent.shape[0], cotangent.shape[1], weight_codes.shape[1], weight_codes.shape[0],
        weight_scale.shape[0], lax.axis_size("intra"), lax.axis_size("inter"),
    )
    got, dgate, dup = main_call(
        plan, gate_pre, up_pre, cotangent, weight_codes, weight_scale, section_one, section_two
    )
    codes_out, dgate, dup = join_call(got, dgate, dup)
    return dgate, dup, codes_out


def solution(mesh):
    placed = (
        P("intra", "inter"),
        P("intra", "inter"),
        P("intra", None),
        P("intra", "inter"),
        P("intra", "inter"),
        P(None, "inter"),
        P("intra", "inter"),
    )
    return jax.shard_map(
        on_device,
        mesh=mesh,
        in_specs=placed,
        out_specs=(P("intra", "inter"), P("intra", "inter"), P(("intra", "inter"), None)),
        check_vma=False,
    )
```

```python
import functools

import jax
import jax.numpy as jnp
from jax import lax
from jax.experimental import pallas as pl
from jax.experimental.pallas import tpu as pltpu
from jax.sharding import PartitionSpec as P

MESH = pl.DeviceIdType.MESH
LANES = 128
PIECE = 512


def times(n, x):
    return pl.multiple_of(x, n)


def bits_below(n):
    return [1 << k for k in range(n.bit_length() - 1)]


def xor(x, y, n):
    out = 0
    for bit in bits_below(n):
        one = lax.rem(lax.div(x, jnp.int32(bit)) + lax.div(jnp.int32(y), jnp.int32(bit)), jnp.int32(2))
        out = out + bit * one
    return out


def combos(masks):
    out = [0]
    for mask in masks:
        out = out + [c ^ mask for c in out]
    return out


def pieces(lo, hi, most=PIECE):
    out = []
    while lo < hi:
        out.append((lo, min(most, hi - lo)))
        lo += most
    return out


class Plan:
    def __init__(self, tok, model, width, rows, n_blocks, n_intra, n_inter):
        self.tok, self.model, self.width, self.rows = tok, model, width, rows
        self.blocks, self.blk = n_blocks, rows // n_blocks
        self.n_intra, self.n_inter = n_intra, n_inter
        self.own = rows // n_inter
        lanes = width // LANES
        self.swap = (lanes + 1) // 2 * LANES
        self.keep = width - self.swap
        self.wide = width + self.swap
        self.half = n_inter // 2
        self.near_rows = rows // 2
        self.quarter = rows // 4
        self.tile = max(self.own, LANES)
        self.share = [[1], [1], [1], [1]]
        self.most_shares = 2
        self.dims = bits_below(n_intra)
        self.far_cols = pieces(0, self.keep)
        self.home_cols = pieces(self.keep, width)
        self.swap_cols = pieces(width, self.wide)
        self.hidden_cols = self.far_cols + self.home_cols + self.swap_cols
        self.sum_cols = pieces(0, width)

    def order(self, color):
        return self.dims[color:] + self.dims[:color]


def remote(src, dst, send, recv, device):
    return pltpu.make_async_remote_copy(
        src_ref=src, dst_ref=dst, send_sem=send, recv_sem=recv, device_id=device, device_id_type=MESH
    )


def main_kernel(
    plan,
    gate_hbm, up_hbm, cot_hbm, codes_hbm, scale_hbm, one_hbm, two_hbm,
    got_hbm, dgate_hbm, dup_hbm,
    gate, up, hid, cols, codes, scale, lay, inv, ratio, coded, part, sums,
    load_sem, xy_sem, share_sem, swap_sem, gather_sem, sum_sem, out_sem, own_sem, store_sem,
):
    p = plan
    i = lax.axis_index("intra")
    b = lax.axis_index("inter")
    n_a, n_b, tok = p.n_intra, p.n_inter, p.tok
    side = lax.div(b, jnp.int32(p.half))
    below = lax.rem(lax.div(b, jnp.int32(p.half // 2)), jnp.int32(2))
    outer = 1 - lax.rem(side + below, jnp.int32(2))
    early = outer * side + (1 - outer) * (1 - side)
    late = 1 - early
    colors = len(p.dims)
    color_tok = tok // colors
    ia = functools.partial(xor, i, n=n_a)
    ib = functools.partial(xor, b, n=n_b)

    loads = [
        pltpu.make_async_copy(gate_hbm, gate, load_sem.at[0]),
        pltpu.make_async_copy(up_hbm, up, load_sem.at[1]),
        pltpu.make_async_copy(
            one_hbm.at[pl.ds(times(8, i * p.blocks), p.blocks)], inv.at[:, :p.width], load_sem.at[2]
        ),
        pltpu.make_async_copy(two_hbm, ratio.at[:, :p.width], load_sem.at[3]),
        pltpu.make_async_copy(
            cot_hbm.at[:, pl.ds(times(LANES, i * p.rows), p.rows)],
            cols.at[pl.ds(times(tok, i * tok), tok)],
            load_sem.at[4],
        ),
        pltpu.make_async_copy(codes_hbm, codes, load_sem.at[5]),
        pltpu.make_async_copy(scale_hbm, scale, load_sem.at[6]),
    ]
    for load in loads:
        load.start()

    barrier = pltpu.get_barrier_semaphore()
    for a in range(1, n_a):
        pl.semaphore_signal(barrier, inc=1, device_id=(ia(a), b), device_id_type=MESH)
    for a in range(1, n_b):
        pl.semaphore_signal(barrier, inc=1, device_id=(i, ib(a)), device_id_type=MESH)
    pl.semaphore_wait(barrier, n_a - 1 + n_b - 1)

    def row_start(toward, q):
        return times(LANES, toward * p.near_rows + q * p.quarter)

    def step_rows(step):
        return row_start(early if step < 2 else late, step % 2)

    def share_of(step):
        n = 1 << len(p.share[step])
        return n, lax.rem(b, jnp.int32(n)), tok // n

    def across(step, a, sending):
        peer = ia(a)
        r0 = step_rows(step)
        _, share_at, part_tok = share_of(step)
        block = i if sending else peer
        src = cot_hbm.at[
            pl.ds(times(16, share_at * part_tok), part_tok),
            pl.ds(times(LANES, peer * p.rows + r0), p.quarter),
        ]
        dst = cols.at[
            pl.ds(times(16, block * tok + share_at * part_tok), part_tok), pl.ds(r0, p.quarter)
        ]
        k = step * (n_a - 1) + a - 1
        return remote(src, dst, xy_sem.at[0, k], xy_sem.at[1, k], (peer, b))

    def start_across(step):
        for a in range(1, n_a):
            across(step, a, True).start()

    def wait_across(step):
        for a in range(1, n_a):
            across(step, a, False).wait_recv()

    def shares(step, phase, sending):
        mask = p.share[step][phase]
        peer = ib(mask)
        r0 = step_rows(step)
        n_share, share_at, part_tok = share_of(step)
        out = []
        for a in range(1, n_a):
            for n, c in enumerate(combos(p.share[step][:phase])):
                at = xor(share_at, c if sending else c ^ mask, n_share)
                ref = cols.at[
                    pl.ds(times(16, ia(a) * tok + at * part_tok), part_tok), pl.ds(r0, p.quarter)
                ]
                k = (step * (n_a - 1) + a - 1) * (p.most_shares - 1) + (1 << phase) - 1 + n
                out.append(remote(ref, ref, share_sem.at[0, k], share_sem.at[1, k], (i, peer)))
        return out

    def start_shares(step, phase):
        for copy in shares(step, phase, True):
            copy.start()

    def wait_shares(step, phase):
        for copy in shares(step, phase, False):
            copy.wait_recv()

    def gathers(piece, phase, sending):
        c0, w = p.hidden_cols[piece]
        out = []
        for color in range(colors):
            order = p.order(color)
            mask = order[phase]
            for n, c in enumerate(combos(order[:phase])):
                block = ia(c if sending else c ^ mask)
                ref = hid.at[
                    pl.ds(times(16, block * tok + color * color_tok), color_tok), c0:c0 + w
                ]
                k = (piece * colors + color) * (n_a - 1) + (1 << phase) - 1 + n
                out.append(remote(ref, ref, gather_sem.at[0, k], gather_sem.at[1, k], (ia(mask), b)))
        return out

    def start_gather(piece, phase):
        for copy in gathers(piece, phase, True):
            copy.start()

    def wait_gather(piece, phase):
        for copy in gathers(piece, phase, False):
            copy.wait_recv()

    def rest_of_gather(piece, phase):
        for q in range(phase, len(p.dims)):
            wait_gather(piece, q)
            if q + 1 < len(p.dims):
                start_gather(piece, q + 1)

    def make_hidden(piece):
        c0, w = p.hidden_cols[piece]
        step_tok = 64

        def body(t, carry):
            rows = pl.ds(times(step_tok, t * step_tok), step_tok)
            g = gate[rows, c0:c0 + w].astype(jnp.float32)
            u = up[rows, c0:c0 + w].astype(jnp.float32)
            h = g * jax.nn.sigmoid(g) * u
            hid[pl.ds(times(step_tok, i * tok + t * step_tok), step_tok), c0:c0 + w] = h.astype(hid.dtype)
            return carry

        lax.fori_loop(0, tok // step_tok, body, 0)

    n_half = p.blocks // 2

    def swaps(sending):
        other = ib(p.half)
        at = (1 - side) if sending else side
        rows = pl.ds(times(8, at * n_half), n_half)
        block = pl.ds(times(tok, i * tok), tok)
        out = []
        k = 0
        for buf, sel in ((hid, block), (inv, rows), (ratio, rows)):
            out.append(
                remote(
                    buf.at[sel, p.keep:p.width], buf.at[sel, p.width:p.wide],
                    swap_sem.at[0, k], swap_sem.at[1, k], (i, other),
                )
            )
            k += 1
        return out

    def prepare_scales():
        one = inv[:, :p.width]
        ratio[:, :p.width] = one / ratio[:, :p.width]
        inv[:, :p.width] = 1.0 / (7.0 * one)

    n_pieces = len(p.hidden_cols)
    per = p.tile // p.own

    def out_copy(owner, piece):
        c0, w = p.hidden_cols[piece]
        if c0 < p.width:
            source, at = b, c0
        else:
            source, at = ib(p.half), c0 - p.swap
        rel = ib(owner)
        k = rel * n_pieces + piece
        return remote(
            coded.at[pl.ds(times(16, owner * p.own), p.own), c0:c0 + w],
            got_hbm.at[source, :, at:at + w],
            out_sem.at[0, k], out_sem.at[1, k], (i, owner),
        )

    def own_copy(piece):
        c0, w = p.hidden_cols[piece]
        if c0 < p.width:
            source, at = b, c0
        else:
            source, at = ib(p.half), c0 - p.swap
        return pltpu.make_async_copy(
            coded.at[pl.ds(times(16, b * p.own), p.own), c0:c0 + w],
            got_hbm.at[source, :, at:at + w],
            own_sem.at[piece],
        )

    def send_tile(start, piece):
        for o in range(per):
            owner = lax.div(start, jnp.int32(p.own)) + o

            @pl.when(owner == b)
            def _():
                own_copy(piece).start()

            @pl.when(owner != b)
            def _():
                out_copy(owner, piece).start()

    def send_coded(toward, q, piece):
        r0 = row_start(toward, q)

        def body(t, carry):
            send_tile(times(p.tile, r0 + t * p.tile), piece)
            return carry

        lax.fori_loop(0, p.quarter // p.tile, body, 0)

    def make_coded(toward, q, piece, now=None):
        c0, w = p.hidden_cols[piece]
        r0 = row_start(toward, q)

        def body(t, carry):
            start = times(p.tile, r0 + t * p.tile)
            total = [None] * (p.tile // p.blk)
            for a in range(n_a):
                term = lax.dot_general(
                    cols[a * tok:(a + 1) * tok, pl.ds(start, p.tile)],
                    hid[a * tok:(a + 1) * tok, c0:c0 + w],
                    (((0,), (0,)), ((), ())),
                    preferred_element_type=jnp.float32,
                )
                for q in range(p.tile // p.blk):
                    at = lax.div(start, jnp.int32(p.blk)) + q
                    v = jnp.tanh(term[q * p.blk:(q + 1) * p.blk] * inv[pl.ds(at, 1), c0:c0 + w])
                    total[q] = v if a == 0 else total[q] + v
            for q in range(p.tile // p.blk):
                at = lax.div(start, jnp.int32(p.blk)) + q
                second = 7.0 * jnp.tanh(total[q] * ratio[pl.ds(at, 1), c0:c0 + w])
                coded[pl.ds(times(p.blk, start + q * p.blk), p.blk), c0:c0 + w] = second.astype(coded.dtype)
            if now is None:
                send_tile(start, piece)
            else:
                pl.when(now)(lambda: send_tile(start, piece))
            return carry

        lax.fori_loop(0, p.quarter // p.tile, body, 0)

    sub = 256 if all(w % 256 == 0 for _, w in p.sum_cols) else LANES

    def make_partial(piece):
        c0, w = p.sum_cols[piece]

        def body(t, carry):
            at = times(LANES, c0 + t * sub)

            def scaled(n, inner):
                rows = pl.ds(times(p.blk, n * p.blk), p.blk)
                lay[rows, :] = (
                    codes[rows, pl.ds(at, sub)].astype(jnp.float32)
                    * scale[pl.ds(n, 1), pl.ds(at, sub)].astype(jnp.float32)
                ).astype(lay.dtype)
                return inner

            for n in range(p.blocks):
                scaled(n, 0)

            def block(a, inner):
                rows = pl.ds(times(tok, a * tok), tok)
                part[rows, pl.ds(at, sub)] = jnp.dot(
                    cols[rows, :], lay[...], preferred_element_type=jnp.float32
                ).astype(part.dtype)
                return inner

            lax.fori_loop(0, n_a, block, 0)
            return carry

        lax.fori_loop(0, w // sub, body, 0)

    def sum_copies(piece, phase, sending):
        c0, w = p.sum_cols[piece]
        out = []
        for color in range(colors):
            order = p.order(color)
            mask = order[phase]
            base = n_a - (n_a >> phase)
            for n, c in enumerate(combos(order[phase + 1:])):
                src = part.at[
                    pl.ds(times(16, ia(c ^ mask) * tok + color * color_tok), color_tok), c0:c0 + w
                ]
                dst = sums.at[
                    (base + n) * tok + color * color_tok:(base + n) * tok + (color + 1) * color_tok,
                    c0:c0 + w,
                ]
                k = (piece * colors + color) * (n_a - 1) + base + n
                out.append(
                    (remote(src, dst, sum_sem.at[0, k], sum_sem.at[1, k], (ia(mask), b)), color, base + n, c)
                )
        return out

    def start_sum(piece, phase):
        for copy, *_ in sum_copies(piece, phase, True):
            copy.start()

    def finish_sum(piece, phase):
        c0, w = p.sum_cols[piece]
        last = phase + 1 == len(p.dims)
        step_tok = 32
        for copy, color, slot, c in sum_copies(piece, phase, False):
            copy.wait_recv()

            def body(t, carry):
                mine = pl.ds(times(16, ia(c) * tok + color * color_tok + t * step_tok), step_tok)
                theirs = pl.ds(times(16, slot * tok + color * color_tok + t * step_tok), step_tok)
                both = part[mine, c0:c0 + w].astype(jnp.float32) + sums[theirs, c0:c0 + w].astype(jnp.float32)
                if not last:
                    part[mine, c0:c0 + w] = both.astype(part.dtype)
                else:
                    here = pl.ds(times(16, color * color_tok + t * step_tok), step_tok)
                    g = gate[here, c0:c0 + w].astype(jnp.float32)
                    u = up[here, c0:c0 + w].astype(jnp.float32)
                    sigma = jax.nn.sigmoid(g)
                    gate[here, c0:c0 + w] = (both * u * sigma * (1.0 + g * (1.0 - sigma))).astype(gate.dtype)
                    up[here, c0:c0 + w] = (both * (g * sigma)).astype(up.dtype)
                return carry

            lax.fori_loop(0, color_tok // step_tok, body, 0)
        if not last:
            start_sum(piece, phase + 1)
        else:
            for copy in stores(piece):
                copy.start()

    def stores(piece):
        c0, w = p.sum_cols[piece]
        return [
            pltpu.make_async_copy(src.at[:, c0:c0 + w], dst.at[:, c0:c0 + w], store_sem.at[2 * piece + n])
            for n, (src, dst) in enumerate(((gate, dgate_hbm), (up, dup_hbm)))
        ]

    far = list(range(len(p.far_cols)))
    home = [len(far) + n for n in range(len(p.home_cols))]
    swapped = [len(far) + len(home) + n for n in range(len(p.swap_cols))]
    n_sum = len(p.sum_cols)
    first = (far + home)[0]
    later_far = [x for x in far if x != first]
    later_home = [x for x in home if x != first]

    def next_gather(piece):
        wait_gather(piece, 0)
        if len(p.dims) > 1:
            start_gather(piece, 1)

    def finish_shares(step, phase=0):
        for n in range(phase, len(p.share[step])):
            wait_shares(step, n)
            if n + 1 < len(p.share[step]):
                start_shares(step, n + 1)

    loads[0].wait()
    loads[1].wait()
    make_hidden(first)
    start_gather(first, 0)
    start_across(0)
    for x in home:
        if x != first:
            make_hidden(x)
    loads[2].wait()
    loads[3].wait()
    prepare_scales()

    def start_swaps():
        for copy in swaps(True):
            copy.start()

    start_swaps()
    for x in later_far:
        make_hidden(x)
    next_gather(first)
    for x in later_far:
        start_gather(x, 0)
    start_across(1)
    loads[4].wait()
    wait_across(0)
    start_shares(0, 0)
    rest_of_gather(first, 1)
    finish_shares(0)
    if far:
        make_coded(early, 0, first)
    for x in later_far:
        next_gather(x)
    start_across(2)
    for x in later_home:
        start_gather(x, 0)
    start_across(3)
    wait_across(1)
    start_shares(1, 0)
    finish_shares(1)
    if far:
        make_coded(early, 1, first)
    for x in later_far:
        rest_of_gather(x, 1)
        make_coded(early, 0, x)
        make_coded(early, 1, x)
    wait_across(2)
    start_shares(2, 0)
    for x in later_home:
        next_gather(x)
    wait_across(3)
    start_shares(3, 0)
    for copy in swaps(False):
        copy.wait_recv()
    for x in swapped:
        start_gather(x, 0)
    finish_shares(2)
    finish_shares(3)
    hold = outer * lax.rem(b, jnp.int32(2))
    for x in far:
        make_coded(late, 0, x, hold == 0)
        make_coded(late, 1, x, hold == 0)
    loads[5].wait()
    loads[6].wait()
    for n in range(n_sum // 2):
        make_partial(n)
    for x in swapped:
        next_gather(x)
    for n in range(n_sum // 2):
        start_sum(n, 0)
    for x in home:
        if x != first:
            rest_of_gather(x, 1)
        make_coded(side, 0, x)
        make_coded(side, 1, x)

    @pl.when(hold == 1)
    def _():
        for x in far:
            send_coded(late, 0, x)
            send_coded(late, 1, x)

    for n in range(n_sum // 2, n_sum):
        make_partial(n)
        start_sum(n, 0)
    for x in swapped:
        rest_of_gather(x, 1)
        make_coded(side, 0, x)
        make_coded(side, 1, x)
    for phase in range(len(p.dims)):
        for n in range(n_sum):
            finish_sum(n, phase)

    for n in range(n_sum):
        for copy in stores(n):
            copy.wait()
    for x in range(n_pieces):
        own_copy(x).wait()
        for rel in range(1, n_b if x in far else p.half):
            owner = ib(rel)
            copy = out_copy(owner, x)
            copy.wait_recv()
            copy.wait_send()
    for step in range(4):
        for a in range(1, n_a):
            across(step, a, True).wait_send()
        for phase in range(len(p.share[step])):
            for copy in shares(step, phase, True):
                copy.wait_send()
    for copy in swaps(True):
        copy.wait_send()
    for phase in range(len(p.dims)):
        for x in range(n_pieces):
            for copy in gathers(x, phase, True):
                copy.wait_send()
        for n in range(n_sum):
            for copy, *_ in sum_copies(n, phase, True):
                copy.wait_send()


def main_call(plan, gate, up, cot, codes, scale, one, two):
    p = plan
    bf16, f32 = jnp.bfloat16, jnp.float32
    vmem, dma = pltpu.VMEM, pltpu.SemaphoreType.DMA
    everywhere = pl.BlockSpec(memory_space=pl.ANY)
    gather = len(p.dims) * (p.n_intra - 1)
    flops = 4 * p.rows * p.width * p.n_intra * p.tok
    return pl.pallas_call(
        functools.partial(main_kernel, p),
        in_specs=[everywhere] * 7,
        out_specs=[everywhere] * 3,
        out_shape=[
            jax.ShapeDtypeStruct((p.n_inter, p.own, p.width), bf16),
            jax.ShapeDtypeStruct((p.tok, p.width), bf16),
            jax.ShapeDtypeStruct((p.tok, p.width), bf16),
        ],
        scratch_shapes=[
            vmem((p.tok, p.width), bf16),
            vmem((p.tok, p.width), bf16),
            vmem((p.n_intra * p.tok, p.wide), bf16),
            vmem((p.n_intra * p.tok, p.rows), bf16),
            vmem((p.rows, p.width), bf16),
            vmem((p.blocks, p.width), bf16),
            vmem((p.rows, 256 if all(w % 256 == 0 for _, w in p.sum_cols) else LANES), bf16),
            vmem((p.blocks, p.wide), f32),
            vmem((p.blocks, p.wide), f32),
            vmem((p.rows, p.wide), bf16),
            vmem((p.n_intra * p.tok, p.width), bf16),
            vmem(((p.n_intra - 1) * p.tok, p.width), bf16),
            dma((7,)),
            dma((2, 4 * (p.n_intra - 1))),
            dma((2, 4 * (p.n_intra - 1) * (p.most_shares - 1))),
            dma((2, 3)),
            dma((2, len(p.hidden_cols) * gather)),
            dma((2, len(p.sum_cols) * gather)),
            dma((2, p.n_inter * len(p.hidden_cols))),
            dma((len(p.hidden_cols),)),
            dma((2 * len(p.sum_cols),)),
        ],
        cost_estimate=pl.CostEstimate(
            flops=flops, bytes_accessed=2 * flops // p.tok, transcendentals=5 * p.rows * p.width
        ),
        compiler_params=pltpu.CompilerParams(
            collective_id=0, has_side_effects=True, vmem_limit_bytes=63 * 2**20
        ),
    )(gate, up, cot, codes, scale, one, two)


def join_kernel(got, dgate, dup, codes_out, dgate_out, dup_out):
    codes_out[...] = got[...].astype(jnp.float32)
    dgate_out[...] = dgate[...]
    dup_out[...] = dup[...]


def join_call(got, dgate, dup):
    sources, rows, width = got.shape
    tok = dgate.shape[0]
    grads = pl.BlockSpec((tok // sources, width), lambda j: (j, 0))
    return pl.pallas_call(
        join_kernel,
        grid=(sources,),
        in_specs=[pl.BlockSpec((None, rows, width), lambda j: (j, 0, 0)), grads, grads],
        out_specs=[pl.BlockSpec((rows, width), lambda j: (0, j)), grads, grads],
        out_shape=[
            jax.ShapeDtypeStruct((rows, sources * width), jnp.float32),
            jax.ShapeDtypeStruct(dgate.shape, dgate.dtype),
            jax.ShapeDtypeStruct(dup.shape, dup.dtype),
        ],
        cost_estimate=pl.CostEstimate(
            flops=0, bytes_accessed=6 * got.size + 8 * dgate.size, transcendentals=0
        ),
        compiler_params=pltpu.CompilerParams(vmem_limit_bytes=63 * 2**20),
    )(got, dgate, dup)


def on_device(gate_pre, up_pre, cotangent, weight_codes, weight_scale, section_one, section_two):
    plan = Plan(
        cotangent.shape[0], cotangent.shape[1], weight_codes.shape[1], weight_codes.shape[0],
        weight_scale.shape[0], lax.axis_size("intra"), lax.axis_size("inter"),
    )
    got, dgate, dup = main_call(
        plan, gate_pre, up_pre, cotangent, weight_codes, weight_scale, section_one, section_two
    )
    codes_out, dgate, dup = join_call(got, dgate, dup)
    return dgate, dup, codes_out


def solution(mesh):
    placed = (
        P("intra", "inter"),
        P("intra", "inter"),
        P("intra", None),
        P("intra", "inter"),
        P("intra", "inter"),
        P(None, "inter"),
        P("intra", "inter"),
    )
    return jax.shard_map(
        on_device,
        mesh=mesh,
        in_specs=placed,
        out_specs=(P("intra", "inter"), P("intra", "inter"), P(("intra", "inter"), None)),
        check_vma=False,
    )
```
